256 devices in a mesh: py: 8 (over z), px: 16 (over y, x), shift: 2 (over core).
Axes of the slice: x: 4, y: 4, z: 8, core: 2. Of those that a mesh axis runs over, the one named last changes fastest.
Arguments:
- right_side: float32 [1024, 1024, 256], P(('shift', 'py'), 'px'), parts along dimension 0, may hold values from -6 to 6
- first_guess: float32 [1024, 1024, 256], P(('shift', 'py'), 'px'), parts along dimension 0, may hold values from -6 to 6
- mass_term: float32 [1024, 1024, 256], P(('shift', 'py'), 'px'), parts along dimension 0, may hold values from 0.1 to 0.9
Outputs:
- corrected: float32 [1024, 1024, 256], P(('shift', 'py'), 'px'), parts along dimension 0
- remaining: float32 [1024, 1024, 256], P(('shift', 'py'), 'px'), parts along dimension 0
The draws below stay inside these ranges and needn't reach their ends.
There are 2 independent parts, one for each index of `shift`. The reference program is written for one: setup_inputs(seed, part) draws one part's arguments, and reference() takes and returns one part's arrays. A program takes and returns all parts, laid end to end along the dimension named above; each array names one. Nothing has to cross between parts.
All inputs are finite; a program needn't handle non-finite values.
Results may differ from the reference program's by a relative error of at most 0.000031.
Values sent between devices are 32-bit elements.
A program may use at most 128 MiB of HBM per device.

```python
import jax
import jax.numpy as jnp
from jax import lax

MEMBERS = 256
RATIO = 4
BEFORE = 2
AFTER = 3
INNER = 9
GRID_Y = 512
GRID_X = 1024


def block_levels(key, shape, shards, low, largest):
    def one(axis_at, blocks):
        heights = jax.random.uniform(jax.random.fold_in(jax.random.fold_in(key, 6), axis_at), (blocks,), jnp.float32, low / len(shards), largest / len(shards))
        return jnp.repeat(jnp.exp(heights), shape[axis_at] // blocks).reshape((-1,) + (1,) * (len(shape) - axis_at - 1))

    gain = one(*shards[0])
    for cut in shards[1:]:
        gain = gain * one(*cut)
    return gain


def bell_draw(stream_key, shape, width, bound, shards=(), dtype=jnp.bfloat16):
    array = jax.random.normal(stream_key, shape, jnp.float32) * width
    if len(shards) > 0:
        array = block_levels(stream_key, shape, shards, -0.22, 0.18) * array
    return jnp.clip(array, min=-bound, max=bound).astype(dtype)


def setup_inputs(seed: int = 0, part: int = 0) -> dict:
    seeds = jax.random.split(jax.random.key(seed), 4)
    part_splits = jax.random.split(jax.random.fold_in(seeds[3], part), 4)
    return {
        "right_side": bell_draw(part_splits[0], (GRID_Y, GRID_X, MEMBERS), 1.0, 6.0, ((0, 8), (1, 16)), jnp.float32),
        "first_guess": bell_draw(part_splits[1], (GRID_Y, GRID_X, MEMBERS), 1.0, 6.0, ((0, 8), (1, 16)), jnp.float32),
        "mass_term": jnp.clip(0.1 + 0.79999997 * jax.random.uniform(part_splits[2], (GRID_Y, GRID_X, MEMBERS), jnp.float32) ** block_levels(part_splits[2], (GRID_Y, GRID_X, MEMBERS), ((0, 8), (1, 16)), -0.2, 0.2), 0.1, 0.9),
    }


def neighbour_sum(padded):
    inner_y, inner_x = padded.shape[0] - 2, padded.shape[1] - 2
    middle_rows = lax.slice_in_dim(padded, 1, 1 + inner_y, axis=0)
    middle_columns = lax.slice_in_dim(padded, 1, 1 + inner_x, axis=1)
    return (lax.slice_in_dim(middle_columns, 0, inner_y, axis=0) + lax.slice_in_dim(middle_columns, 2, 2 + inner_y, axis=0)
            + lax.slice_in_dim(middle_rows, 0, inner_x, axis=1) + lax.slice_in_dim(middle_rows, 2, 2 + inner_x, axis=1))


def sweep_once(padded, values, load, mass_here):
    return values + 0.8 * (load + neighbour_sum(padded) - (4.0 + mass_here) * values) / (4.0 + mass_here)


def block_means(values):
    cut = values.reshape(values.shape[0] // RATIO, RATIO, values.shape[1] // RATIO, RATIO, values.shape[2])
    return jnp.mean(cut, axis=(1, 3))


def spread_blocks(values):
    return jnp.repeat(jnp.repeat(values, RATIO, axis=0), RATIO, axis=1)


def reference(right_side, first_guess, mass_term):
    values = first_guess
    for sweep in range(BEFORE):
        values = sweep_once(jnp.pad(values, ((1, 1), (1, 1), (0, 0)), mode="wrap"), values, right_side, mass_term)
    defect = right_side + neighbour_sum(jnp.pad(values, ((1, 1), (1, 1), (0, 0)), mode="wrap")) - (4.0 + mass_term) * values
    coarse_load, coarse_mass = block_means(defect) * RATIO, block_means(mass_term) * RATIO
    coarse_values = jnp.zeros_like(coarse_load)
    for sweep in range(INNER):
        coarse_values = sweep_once(jnp.pad(coarse_values, ((1, 1), (1, 1), (0, 0)), mode="wrap"), coarse_values, coarse_load, coarse_mass)
    values = values + spread_blocks(coarse_values)
    for sweep in range(AFTER):
        values = sweep_once(jnp.pad(values, ((1, 1), (1, 1), (0, 0)), mode="wrap"), values, right_side, mass_term)
    corrected = values
    remaining = right_side + neighbour_sum(jnp.pad(corrected, ((1, 1), (1, 1), (0, 0)), mode="wrap")) - (4.0 + mass_term) * corrected
    return corrected, remaining
```

```python
import jax
import jax.numpy as jnp
from jax import lax
from jax.experimental import pallas as pl
from jax.experimental.pallas import tpu as pltpu
from jax.sharding import PartitionSpec as P

RATIO = 4
H, L = 2, 128
B = 64
C = B // RATIO
Y0, X0, YS, XS = 4, 12, 72, 88
D = 9
CX0, CXS = 11, 40
EX0, EXS = 8, 104
ANY = pl.BlockSpec(memory_space=pl.ANY)
VMEM = pl.BlockSpec(memory_space=pltpu.VMEM)
FINE = (H, YS, XS, L)
COARSE = (H, C + 2 * D, CXS, L)
SPREAD = (H, C + 4, EXS, L)


def tiles(first, last):
    starts = list(range(first, last - 7, 8))
    if starts[-1] + 8 < last:
        starts.append(last - 8)
    return starts


def group_of(count, best=(4, 6, 5, 3, 2)):
    return next(g for g in (*best, 1) if count % g == 0)


def rows_loop(first, last, body, best=(4, 6, 5, 3, 2)):
    g = group_of(last - first, best)

    def step(i, carry):
        body(first + i * g, g)
        return carry

    lax.fori_loop(0, (last - first) // g, step, 0)


def near_sum(src, h, y, x, g):
    column = [src[h, y + k, pl.ds(x, 8), :] for k in range(-1, g + 1)]
    sums = []
    for k in range(g):
        left = src[h, y + k, pl.ds(x - 1, 8), :]
        right = src[h, y + k, pl.ds(x + 1, 8), :]
        sums.append((column[k] + column[k + 2]) + (left + right))
    return column[1:-1], sums


def sweep(dst, src, load, weight, ys, xs, y0=Y0, x0=X0):
    def body(y, g):
        for h in range(H):
            for x in tiles(*xs):
                centre, near = near_sum(src, h, y + y0, x + x0, g)
                for k in range(g):
                    at = (h, y + y0 + k, pl.ds(x + x0, 8), slice(None))
                    dst[at] = 0.2 * centre[k] + weight[at] * (load[at] + near[k])

    rows_loop(*ys, body)


def weigh(dst, mass, ys, xs, y0=Y0, x0=X0, best=(4, 6, 5, 3, 2)):
    def body(y, g):
        for h in range(H):
            for x in tiles(*xs):
                for k in range(g):
                    at = (h, y + y0 + k, pl.ds(x + x0, 8), slice(None))
                    dst[at] = 0.8 / (4.0 + mass[at])

    rows_loop(*ys, body, best)


def block_sums(dst, sums):
    def body(y, g):
        for k in range(g):
            for h in range(H):
                for t in range(C // 8):
                    parts = [sums[y + k, h, pl.ds(32 * t + j, 8, stride=4), :] for j in range(4)]
                    dst[h, y + k + D, pl.ds(CX0 + 8 * t, 8), :] = 0.25 * (
                        (parts[0] + parts[1]) + (parts[2] + parts[3])
                    )

    rows_loop(0, C, body)


class Halo:
    def __init__(self, buffer, size, y0, x0, depths, corners, around, send, recv, base):
        self.copies = []
        lo, hi = depths

        def add(dy, dx, ys, xs):
            src = buffer.at[:, pl.ds(y0 + ys[0], ys[1]), pl.ds(x0 + xs[0], xs[1]), :]
            dst = buffer.at[
                :, pl.ds(y0 + ys[0] - dy * size, ys[1]), pl.ds(x0 + xs[0] - dx * size, xs[1]), :
            ]
            n = base + len(self.copies)
            self.copies.append(
                pltpu.make_async_remote_copy(
                    src_ref=src,
                    dst_ref=dst,
                    send_sem=send.at[n],
                    recv_sem=recv.at[n],
                    device_id=around(dy, dx),
                    device_id_type=pl.DeviceIdType.MESH,
                )
            )

        def span(d, low, high):
            return (size - high, high - low) if d > 0 else (low, high - low)

        for (ya, yb), (xa, xb) in corners:
            for dy in (1, -1):
                for dx in (1, -1):
                    add(dy, dx, span(dy, ya, yb), span(dx, xa, xb))
        for d in (1, -1):
            add(0, d, (0, size), span(d, lo, hi))
        for d in (1, -1):
            add(d, 0, span(d, lo, hi), (0, size))

    def start(self):
        for c in self.copies:
            c.start()

    def arrive(self):
        for c in self.copies:
            c.wait_recv()

    def sent(self):
        for c in self.copies:
            c.wait_send()


def first_kernel(
    right, guess, mass, v3, r, w, e, m, u, v1, v2, cl, cm, cw, ca, cb, sums, local, send, recv
):
    npy, npx = lax.axis_size("py"), lax.axis_size("px")
    py, px = lax.axis_index("py"), lax.axis_index("px")

    def around(dy, dx):
        return {"py": lax.rem(py + dy + npy, npy), "px": lax.rem(px + dx + npx, npx)}

    loads = []
    for i, (src, dst) in enumerate(((guess, u), (right, r), (mass, m))):
        loads.append(
            [
                pltpu.make_async_copy(
                    src.at[:, :, pl.ds(h * L, L)],
                    dst.at[h, pl.ds(Y0, B), pl.ds(X0, B), :],
                    local.at[i, h],
                )
                for h in range(H)
            ]
        )
        for c in loads[-1]:
            c.start()

    barrier = pltpu.get_barrier_semaphore()
    ring = [(dy, dx) for dy in (-1, 0, 1) for dx in (-1, 0, 1) if (dy, dx) != (0, 0)]
    for dy, dx in ring:
        pl.semaphore_signal(
            barrier, inc=1, device_id=around(dy, dx), device_id_type=pl.DeviceIdType.MESH
        )
    pl.semaphore_wait(barrier, len(ring))

    halos = []

    def halo(buffer, size, y0, x0, depths, corners):
        base = sum(len(one.copies) for one in halos)
        halos.append(Halo(buffer, size, y0, x0, depths, corners, around, send, recv, base))
        return halos[-1]

    square = lambda n: [((0, n), (0, n))]
    fine = lambda buffer, depths, corners: halo(buffer, B, Y0, X0, depths, corners)
    wedge = [((0, 4), (0, 8)), ((4, 8), (0, 4))]

    for c in loads[0]:
        c.wait()
    u_halo = fine(u, (0, 3), square(2))
    u_halo.start()
    for c in loads[1]:
        c.wait()
    r_halo = fine(r, (0, 2), square(2))
    r_halo.start()
    for c in loads[2]:
        c.wait()
    m_halo = fine(m, (0, 2), square(2))
    m_halo.start()

    def mass_rows(y, g):
        for k in range(g):
            for h in range(H):
                for x in tiles(0, B):
                    parts = [m[h, Y0 + 4 * (y + k) + j, pl.ds(X0 + x, 8), :] for j in range(4)]
                    sums[y + k, h, pl.ds(x, 8), :] = (parts[0] + parts[1]) + (parts[2] + parts[3])

    rows_loop(0, C, mass_rows, (2,))
    block_sums(cm, sums)
    cm_halo = halo(cm, C, D, CX0, (0, D), wedge)
    cm_halo.start()
    r_more = fine(r, (2, 3), [])
    r_more.start()
    m_more = fine(m, (2, 3), [])
    m_more.start()

    weigh(w, m, (0, B), (0, B))

    u_halo.arrive()
    r_halo.arrive()
    m_halo.arrive()
    weigh(w, m, (-2, 0), (-2, B + 2))
    weigh(w, m, (B, B + 2), (-2, B + 2))
    weigh(w, m, (0, B), (-2, 6))
    weigh(w, m, (0, B), (B - 6, B + 2))
    sweep(v1, u, r, w, (-2, B + 2), (-2, B + 2))
    sweep(v2, v1, r, w, (0, B), (-1, B + 1))
    sweep(v2, v1, r, w, (-1, 0), (0, B))
    sweep(v2, v1, r, w, (B, B + 1), (0, B))

    def defect_rows(y, g):
        for h in range(H):
            for x in tiles(0, B):
                centre, near = near_sum(v2, h, Y0 + 4 * y, X0 + x, 4)
                parts = []
                for k in range(4):
                    at = (h, Y0 + 4 * y + k, pl.ds(X0 + x, 8), slice(None))
                    parts.append(r[at] + near[k] - (4.0 + m[at]) * centre[k])
                sums[y, h, pl.ds(x, 8), :] = (parts[0] + parts[1]) + (parts[2] + parts[3])

    rows_loop(0, C, defect_rows, (1,))
    block_sums(cl, sums)
    cl_halo = halo(cl, C, D, CX0, (0, D), wedge)
    cl_halo.start()
    v2_halo = fine(v2, (1, 4), square(3))
    v2_halo.start()

    cm_halo.arrive()
    weigh(cw, cm, (-D, C + D), (-D, C + D), D, CX0)
    cl_halo.arrive()

    def first_coarse(y, g):
        for h in range(H):
            for x in tiles(-D, C + D):
                for k in range(g):
                    at = (h, y + D + k, pl.ds(x + CX0, 8), slice(None))
                    ca[at] = cw[at] * cl[at]

    rows_loop(-D, C + D, first_coarse, (2,))
    here, there = ca, cb
    for n in range(D - 1, 0, -1):
        sweep(there, here, cl, cw, (-n, C + n), (-n, C + n), D, CX0)
        here, there = there, here

    def spread(y, g):
        for k in range(g):
            for h in range(H):
                for t in range(3):
                    value = here[h, y + k + D, pl.ds(CX0 - 1 + 8 * t, 8), :]
                    for j in range(4):
                        e[h, y + k + 2, pl.ds(EX0 - 4 + 32 * t + j, 8, stride=4), :] = value

    rows_loop(-1, C + 1, spread, (2,))

    r_more.arrive()
    m_more.arrive()
    v2_halo.arrive()
    weigh(w, m, (-3, -2), (-3, B + 3), best=(1,))
    weigh(w, m, (B + 2, B + 3), (-3, B + 3), best=(1,))
    weigh(w, m, (-2, B + 2), (-3, 5))
    weigh(w, m, (-2, B + 2), (B - 5, B + 3))
    sweep(v3, v2, r, w, (-3, B + 3), (-3, B + 3))
    for one in halos:
        one.sent()


def second_kernel(v3, r, w, e, mass, corrected, remaining, a, b, m, sem, local):
    loads = [
        pltpu.make_async_copy(mass.at[:, :, pl.ds(h * L, L)], m.at[h], local.at[h])
        for h in range(H)
    ]
    for c in loads:
        c.start()

    def correct(y, g):
        for h in range(H):
            for x in tiles(-4, B + 4):
                at = lambda n, s=0: e[h, y + 2 + n, pl.ds(EX0 + x + s, 8), :]
                here, up, down = at(0), at(-1), at(1)
                sides = at(0, -1) + at(0, 1)
                small = 0.2 * here
                near = [sides + (up + here)] + [sides + (here + here)] * 2 + [sides + (here + down)]
                for k in range(4):
                    cell = (h, Y0 + 4 * y + k, pl.ds(X0 + x, 8), slice(None))
                    a[cell] = v3[cell] + (small + w[cell] * near[k])

    rows_loop(-1, C + 1, correct, (1,))
    sweep(b, a, r, w, (-2, B + 2), (-2, B + 2))
    sweep(a, b, r, w, (-1, B + 1), (-1, B + 1))

    copies = []

    def put(src, dst, i, first, count):
        for h in range(H):
            c = pltpu.make_async_copy(
                src.at[h, pl.ds(Y0 + first, count), pl.ds(X0, B), :],
                dst.at[pl.ds(first, count), :, pl.ds(h * L, L)],
                sem.at[i, h],
            )
            c.start()
            copies.append(c)

    put(a, corrected, 0, 0, B)

    def rest(y, g):
        for h in range(H):
            for x in tiles(0, B):
                centre, near = near_sum(a, h, Y0 + y, X0 + x, g)
                for k in range(g):
                    at = (h, Y0 + y + k, pl.ds(X0 + x, 8), slice(None))
                    heavy = 4.0 + m[h, y + k, pl.ds(x, 8), :]
                    b[at] = r[at] + near[k] - heavy * centre[k]

    for c in loads:
        c.wait()
    for q in range(4):
        rows_loop(16 * q, 16 * q + 16, rest)
        put(b, remaining, 1 + q, 16 * q, 16)
    for c in copies:
        c.wait()


def shards(right_side, first_guess, mass_term):
    f32 = jnp.float32
    copies = 4 * 8 + 2 * 12 + 2 * 4
    held = pl.pallas_call(
        first_kernel,
        out_shape=(*[pltpu.VMEM(FINE, f32)] * 3, pltpu.VMEM(SPREAD, f32)),
        in_specs=[ANY] * 3,
        out_specs=(VMEM,) * 4,
        scratch_shapes=[
            *[pltpu.VMEM(FINE, f32)] * 4,
            *[pltpu.VMEM(COARSE, f32)] * 5,
            pltpu.VMEM((C, H, B, L), f32),
            pltpu.SemaphoreType.DMA((3, H)),
            pltpu.SemaphoreType.DMA((copies,)),
            pltpu.SemaphoreType.DMA((copies,)),
        ],
        compiler_params=pltpu.CompilerParams(
            collective_id=0, has_side_effects=True, vmem_limit_bytes=40 << 20
        ),
        name="first",
    )(right_side, first_guess, mass_term)
    held = [pltpu.with_memory_space_constraint(one, pltpu.VMEM) for one in held]
    mass_term = pltpu.with_memory_space_constraint(mass_term, pltpu.HBM)
    block = jax.ShapeDtypeStruct(right_side.shape, f32)
    return pl.pallas_call(
        second_kernel,
        out_shape=(block, block),
        in_specs=[VMEM] * 4 + [ANY],
        out_specs=(ANY, ANY),
        scratch_shapes=[
            *[pltpu.VMEM(FINE, f32)] * 2,
            pltpu.VMEM((H, B, B, L), f32),
            pltpu.SemaphoreType.DMA((5, H)),
            pltpu.SemaphoreType.DMA((H,)),
        ],
        compiler_params=pltpu.CompilerParams(vmem_limit_bytes=40 << 20),
        name="second",
    )(*held, mass_term)


def solution(mesh):
    spec = P(("shift", "py"), "px", None)
    return jax.shard_map(
        shards, mesh=mesh, in_specs=(spec,) * 3, out_specs=(spec,) * 2, check_vma=False
    )
```

```python
import jax
import jax.numpy as jnp
from jax import lax
from jax.experimental import pallas as pl
from jax.experimental.pallas import tpu as pltpu
from jax.sharding import PartitionSpec as P

RATIO = 4
H, L = 2, 128
B = 64
C = B // RATIO
Y0, X0, YS, XS = 4, 12, 72, 88
D = 9
CX0, CXS = 11, 40
EX0, EXS = 8, 104
FIRST_CUTS, LAST_CUTS = (23, 47, B + 1), (24, 48, 60, B)
ANY = pl.BlockSpec(memory_space=pl.ANY)
VMEM = pl.BlockSpec(memory_space=pltpu.VMEM)
FINE = (H, YS, XS, L)
COARSE = (H, C + 2 * D, CXS, L)
SPREAD = (H, C + 4, EXS, L)


def tiles(first, last):
    starts = list(range(first, last - 7, 8))
    if starts[-1] + 8 < last:
        starts.append(last - 8)
    return starts


def rows_loop(first, last, body, g=4):
    whole = (last - first) // g

    def step(i, carry):
        body(first + i * g, g)
        return carry

    if whole > 1:
        lax.fori_loop(0, whole, step, 0)
    elif whole:
        body(first, g)
    if (last - first) % g:
        body(first + whole * g, (last - first) % g)


def near_sum(src, h, y, x, g):
    column = [src[h, y + k, pl.ds(x, 8), :] for k in range(-1, g + 1)]
    sums = []
    for k in range(g):
        left = src[h, y + k, pl.ds(x - 1, 8), :]
        right = src[h, y + k, pl.ds(x + 1, 8), :]
        sums.append((column[k] + column[k + 2]) + (left + right))
    return column[1:-1], sums


def sweep(dst, src, load, weight, ys, xs, y0=Y0, x0=X0):
    def body(y, g):
        for h in range(H):
            for x in tiles(*xs):
                centre, near = near_sum(src, h, y + y0, x + x0, g)
                for k in range(g):
                    at = (h, y + y0 + k, pl.ds(x + x0, 8), slice(None))
                    dst[at] = 0.2 * centre[k] + weight[at] * (load[at] + near[k])

    rows_loop(*ys, body)


def weigh(dst, mass, ys, xs, y0=Y0, x0=X0, g=4):
    def body(y, g):
        for h in range(H):
            for x in tiles(*xs):
                for k in range(g):
                    at = (h, y + y0 + k, pl.ds(x + x0, 8), slice(None))
                    dst[at] = 0.8 / (4.0 + mass[at])

    rows_loop(*ys, body, g)


def block_sums(dst, sums, ys):
    def body(y, g):
        for k in range(g):
            for h in range(H):
                for t in range(C // 8):
                    parts = [sums[y + k, h, pl.ds(32 * t + j, 8, stride=4), :] for j in range(4)]
                    dst[h, y + k + D, pl.ds(CX0 + 8 * t, 8), :] = 0.25 * (
                        (parts[0] + parts[1]) + (parts[2] + parts[3])
                    )

    rows_loop(*ys, body)


class Halo:
    def __init__(self, around, send, recv, halos):
        self.around, self.send, self.recv = around, send, recv
        self.base = sum(len(one.copies) for one in halos)
        self.copies = []
        halos.append(self)

    def add(self, buffer, size, y0, x0, dy, dx, ys, xs):
        n = self.base + len(self.copies)
        self.copies.append(
            pltpu.make_async_remote_copy(
                src_ref=buffer.at[:, pl.ds(y0 + ys[0], ys[1]), pl.ds(x0 + xs[0], xs[1]), :],
                dst_ref=buffer.at[
                    :, pl.ds(y0 + ys[0] - dy * size, ys[1]), pl.ds(x0 + xs[0] - dx * size, xs[1]), :
                ],
                send_sem=self.send.at[n],
                recv_sem=self.recv.at[n],
                device_id=self.around(dy, dx),
                device_id_type=pl.DeviceIdType.MESH,
            )
        )

    def edges(self, buffer, size, y0, x0, depths, along):
        low, high = depths
        along = (along[0], along[1] - along[0])
        for d in (1, -1):
            across = (size - high if d > 0 else low, high - low)
            self.add(buffer, size, y0, x0, 0, d, along, across)
            self.add(buffer, size, y0, x0, d, 0, across, along)

    def corners(self, buffer, size, y0, x0, rectangles):
        for (ya, yb), (xa, xb) in rectangles:
            for dy in (1, -1):
                for dx in (1, -1):
                    ys = (size - yb if dy > 0 else ya, yb - ya)
                    xs = (size - xb if dx > 0 else xa, xb - xa)
                    self.add(buffer, size, y0, x0, dy, dx, ys, xs)

    def start(self):
        for c in self.copies:
            c.start()

    def arrive(self):
        for c in self.copies:
            c.wait_recv()

    def sent(self):
        for c in self.copies:
            c.wait_send()


def first_kernel(
    right, guess, mass, v3, r, w, e, m, u, v1, v2, cl, cm, cw, ca, cb, sums, local, send, recv
):
    npy, npx = lax.axis_size("py"), lax.axis_size("px")
    py, px = lax.axis_index("py"), lax.axis_index("px")

    def around(dy, dx):
        return {"py": lax.rem(py + dy + npy, npy), "px": lax.rem(px + dx + npx, npx)}

    pieces = [((0, 4), (0, B)), ((B - 4, B), (0, B)), ((4, B - 4), (0, 8)), ((4, B - 4), (B - 8, B))]
    parts = [pieces, [((4, B - 4), (8, B - 8))]]
    whole = [[((0, B), (0, B))], []]
    loads = {}
    for part in range(2):
        for i, (src, dst) in enumerate(((guess, u), (right, r), (mass, m))):
            loads[i, part] = [
                pltpu.make_async_copy(
                    src.at[pl.ds(ya, yb - ya), pl.ds(xa, xb - xa), pl.ds(h * L, L)],
                    dst.at[h, pl.ds(Y0 + ya, yb - ya), pl.ds(X0 + xa, xb - xa), :],
                    local.at[i, 4 * part + n, h],
                )
                for n, ((ya, yb), (xa, xb)) in enumerate(whole[part])
                for h in range(H)
            ]
    for key in ((0, 0), (1, 0), (2, 0), (0, 1)):
        for c in loads[key]:
            c.start()

    def loaded(i, part):
        for c in loads[i, part]:
            c.wait()

    barrier = pltpu.get_barrier_semaphore()
    ring = [(dy, dx) for dy in (-1, 0, 1) for dx in (-1, 0, 1) if (dy, dx) != (0, 0)]
    for dy, dx in ring:
        pl.semaphore_signal(
            barrier, inc=1, device_id=around(dy, dx), device_id_type=pl.DeviceIdType.MESH
        )
    pl.semaphore_wait(barrier, len(ring))

    halos = []

    def halo(buffer, size, y0, x0, depths, rectangles):
        one = Halo(around, send, recv, halos)
        one.corners(buffer, size, y0, x0, rectangles)
        one.edges(buffer, size, y0, x0, depths, (0, size))
        return one

    square = lambda n: [((0, n), (0, n))]
    fine = lambda buffer, depths, rectangles: halo(buffer, B, Y0, X0, depths, rectangles)
    wedge = [((n, min(n + 2, D)), (0, D - n)) for n in range(0, D, 2)]

    loaded(0, 0)
    u_halo = fine(u, (0, 3), square(2))
    u_halo.start()
    loaded(1, 0)
    r_halo = fine(r, (0, 2), square(2))
    r_halo.start()
    loaded(2, 0)
    m_halo = fine(m, (0, 2), square(2))
    m_halo.start()

    def mass_rows(y, g):
        for k in range(g):
            for h in range(H):
                for x in tiles(0, B):
                    parts = [m[h, Y0 + 4 * (y + k) + j, pl.ds(X0 + x, 8), :] for j in range(4)]
                    sums[y + k, h, pl.ds(x, 8), :] = (parts[0] + parts[1]) + (parts[2] + parts[3])

    loaded(2, 1)
    rows_loop(0, C, mass_rows, 1)
    block_sums(cm, sums, (0, C))
    cm_halo = halo(cm, C, D, CX0, (0, D), wedge)
    cm_halo.start()
    m_more = fine(m, (2, 3), [])
    m_more.start()

    def defect(ys, xs):
        def body(y, g):
            for k in range(g):
                for h in range(H):
                    for x in tiles(*xs):
                        centre, near = near_sum(v2, h, Y0 + 4 * (y + k), X0 + x, 4)
                        parts = []
                        for j in range(4):
                            at = (h, Y0 + 4 * (y + k) + j, pl.ds(X0 + x, 8), slice(None))
                            parts.append(r[at] + near[j] - (4.0 + m[at]) * centre[j])
                        sums[y + k, h, pl.ds(x, 8), :] = (parts[0] + parts[1]) + (
                            parts[2] + parts[3]
                        )

        rows_loop(*ys, body, 1)

    weigh(w, m, (0, B), (0, B))
    loaded(0, 1)
    loaded(1, 1)
    sweep(v1, u, r, w, (2, B - 2), (2, B - 2))
    sweep(v2, v1, r, w, (3, B - 3), (3, B - 3))
    defect((1, C - 1), (4, B - 4))

    u_halo.arrive()
    r_halo.arrive()
    m_halo.arrive()
    for ys in ((-2, 0), (B, B + 2)):
        weigh(w, m, ys, (-2, B + 2))
    for xs in ((-2, 6), (B - 6, B + 2)):
        weigh(w, m, (0, B), xs)
    for ys in ((-2, 2), (B - 2, B + 2)):
        sweep(v1, u, r, w, ys, (-2, B + 2))
    for xs in ((-2, 6), (B - 6, B + 2)):
        sweep(v1, u, r, w, (2, B - 2), xs)
    for ys in ((-1, 3), (B - 3, B + 1)):
        sweep(v2, v1, r, w, ys, (0, B))
    for xs in ((-1, 7), (B - 7, B + 1)):
        sweep(v2, v1, r, w, (0, B), xs)
    for ys in ((0, 1), (C - 1, C)):
        defect(ys, (0, B))
    for xs in ((0, 8), (B - 8, B)):
        defect((1, C - 1), xs)
    block_sums(cl, sums, (0, C))
    cl_halo = halo(cl, C, D, CX0, (0, D), wedge)
    cl_halo.start()

    sweep(v3, v2, r, w, (0, B), (0, B))
    v3_halo = fine(v3, (0, 3), square(2))
    v3_halo.start()
    cm_halo.arrive()
    weigh(cw, cm, (-D, C + D), (-D, C + D), D, CX0)
    cl_halo.arrive()

    def first_coarse(y, g):
        for h in range(H):
            for x in tiles(-D, C + D):
                for k in range(g):
                    at = (h, y + D + k, pl.ds(x + CX0, 8), slice(None))
                    ca[at] = cw[at] * cl[at]

    rows_loop(-D, C + D, first_coarse, 2)
    here, there = ca, cb
    for n in range(D - 1, 0, -1):
        sweep(there, here, cl, cw, (-n, C + n), (-n, C + n), D, CX0)
        here, there = there, here

    def spread(y, g):
        for k in range(g):
            for h in range(H):
                for t in range(3):
                    value = here[h, y + k + D, pl.ds(CX0 - 1 + 8 * t, 8), :]
                    for j in range(4):
                        e[h, y + k + 2, pl.ds(EX0 - 4 + 32 * t + j, 8, stride=4), :] = value

    rows_loop(-1, C + 1, spread, 1)

    m_more.arrive()
    for ys in ((-3, -2), (B + 2, B + 3)):
        weigh(w, m, ys, (0, B))
    for xs in ((-3, 5), (B - 5, B + 3)):
        weigh(w, m, (0, B), xs)
    v3_halo.arrive()
    for one in halos:
        one.sent()


def second_kernel(v3, r, w, e, mass, corrected, remaining, a, b, m, sem, local):
    loads = [
        pltpu.make_async_copy(mass.at[:, :, pl.ds(h * L, L)], m.at[h], local.at[h])
        for h in range(H)
    ]
    for c in loads:
        c.start()

    def correct(y, g):
        for h in range(H):
            for x in tiles(-4, B + 4):
                at = lambda n, s=0: e[h, y + 2 + n, pl.ds(EX0 + x + s, 8), :]
                here, up, down = at(0), at(-1), at(1)
                sides = at(0, -1) + at(0, 1)
                small = 0.2 * here
                near = [sides + (up + here)] + [sides + (here + here)] * 2 + [sides + (here + down)]
                for k in range(4):
                    cell = (h, Y0 + 4 * y + k, pl.ds(X0 + x, 8), slice(None))
                    a[cell] = v3[cell] + (small + w[cell] * near[k])

    rows_loop(-1, C + 1, correct, 1)
    sweep(b, a, r, w, (-2, B + 2), (-2, B + 2))
    copies = []

    def put(src, dst, i, first, count):
        for h in range(H):
            c = pltpu.make_async_copy(
                src.at[h, pl.ds(Y0 + first, count), pl.ds(X0, B), :],
                dst.at[pl.ds(first, count), :, pl.ds(h * L, L)],
                sem.at[i, h],
            )
            c.start()
            copies.append(c)

    last = -1
    for i, upto in enumerate(FIRST_CUTS):
        sweep(a, b, r, w, (last, upto), (-1, B + 1))
        put(a, corrected, i, max(last, 0), min(upto, B) - max(last, 0))
        last = upto

    def rest(y, g):
        for h in range(H):
            for x in tiles(0, B):
                centre, near = near_sum(a, h, Y0 + y, X0 + x, g)
                for k in range(g):
                    at = (h, Y0 + y + k, pl.ds(X0 + x, 8), slice(None))
                    heavy = 4.0 + m[h, y + k, pl.ds(x, 8), :]
                    b[at] = r[at] + near[k] - heavy * centre[k]

    for c in loads:
        c.wait()
    last = 0
    for i, upto in enumerate(LAST_CUTS):
        rows_loop(last, upto, rest)
        put(b, remaining, len(FIRST_CUTS) + i, last, upto - last)
        last = upto
    for c in copies:
        c.wait()


def shards(right_side, first_guess, mass_term):
    f32 = jnp.float32
    copies = 4 * 8 + 2 * 24 + 4
    held = pl.pallas_call(
        first_kernel,
        out_shape=(*[pltpu.VMEM(FINE, f32)] * 3, pltpu.VMEM(SPREAD, f32)),
        in_specs=[ANY] * 3,
        out_specs=(VMEM,) * 4,
        scratch_shapes=[
            *[pltpu.VMEM(FINE, f32)] * 4,
            *[pltpu.VMEM(COARSE, f32)] * 5,
            pltpu.VMEM((C, H, B, L), f32),
            pltpu.SemaphoreType.DMA((3, 5, H)),
            pltpu.SemaphoreType.DMA((copies,)),
            pltpu.SemaphoreType.DMA((copies,)),
        ],
        compiler_params=pltpu.CompilerParams(
            collective_id=0, has_side_effects=True, vmem_limit_bytes=40 << 20
        ),
        name="first",
    )(right_side, first_guess, mass_term)
    held = [pltpu.with_memory_space_constraint(one, pltpu.VMEM) for one in held]
    mass_term = pltpu.with_memory_space_constraint(mass_term, pltpu.HBM)
    block = jax.ShapeDtypeStruct(right_side.shape, f32)
    return pl.pallas_call(
        second_kernel,
        out_shape=(block, block),
        in_specs=[VMEM] * 4 + [ANY],
        out_specs=(ANY, ANY),
        scratch_shapes=[
            *[pltpu.VMEM(FINE, f32)] * 2,
            pltpu.VMEM((H, B, B, L), f32),
            pltpu.SemaphoreType.DMA((len(FIRST_CUTS) + len(LAST_CUTS), H)),
            pltpu.SemaphoreType.DMA((H,)),
        ],
        compiler_params=pltpu.CompilerParams(vmem_limit_bytes=40 << 20),
        name="second",
    )(*held, mass_term)


def solution(mesh):
    spec = P(("shift", "py"), "px", None)
    return jax.shard_map(
        shards, mesh=mesh, in_specs=(spec,) * 3, out_specs=(spec,) * 2, check_vma=False
    )
```

```python
import jax
import jax.numpy as jnp
from jax import lax
from jax.experimental import pallas as pl
from jax.experimental.pallas import tpu as pltpu
from jax.sharding import PartitionSpec as P

RATIO = 4
H, L = 2, 128
B = 64
C = B // RATIO
Y0, X0, YS, XS = 4, 12, 72, 88
D = 9
CX0, CXS = 11, 40
EX0, EXS = 8, 104
FIRST_CUTS, LAST_CUTS = (23, 47, B + 1), (24, 48, 60, B)
ANY = pl.BlockSpec(memory_space=pl.ANY)
VMEM = pl.BlockSpec(memory_space=pltpu.VMEM)
FINE = (H, YS, XS, L)
COARSE = (H, C + 2 * D, CXS, L)
SPREAD = (H, C + 4, EXS, L)


def tiles(first, last):
    starts = list(range(first, last - 7, 8))
    if starts[-1] + 8 < last:
        starts.append(last - 8)
    return starts


def rows_loop(first, last, body, g=4):
    whole = (last - first) // g

    def step(i, carry):
        body(first + i * g, g)
        return carry

    if whole > 1:
        lax.fori_loop(0, whole, step, 0)
    elif whole:
        body(first, g)
    if (last - first) % g:
        body(first + whole * g, (last - first) % g)


def near_sum(src, h, y, x, g):
    column = [src[h, y + k, pl.ds(x, 8), :] for k in range(-1, g + 1)]
    sums = []
    for k in range(g):
        left = src[h, y + k, pl.ds(x - 1, 8), :]
        right = src[h, y + k, pl.ds(x + 1, 8), :]
        sums.append((column[k] + column[k + 2]) + (left + right))
    return column[1:-1], sums


def sweep(dst, src, load, weight, ys, xs, y0=Y0, x0=X0):
    def body(y, g):
        for h in range(H):
            for x in tiles(*xs):
                centre, near = near_sum(src, h, y + y0, x + x0, g)
                for k in range(g):
                    at = (h, y + y0 + k, pl.ds(x + x0, 8), slice(None))
                    dst[at] = 0.2 * centre[k] + weight[at] * (load[at] + near[k])

    rows_loop(*ys, body)


def weigh(dst, mass, ys, xs, y0=Y0, x0=X0, g=4):
    def body(y, g):
        for h in range(H):
            for x in tiles(*xs):
                for k in range(g):
                    at = (h, y + y0 + k, pl.ds(x + x0, 8), slice(None))
                    dst[at] = 0.8 / (4.0 + mass[at])

    rows_loop(*ys, body, g)


def block_sums(dst, sums, ys):
    def body(y, g):
        for k in range(g):
            for h in range(H):
                for t in range(C // 8):
                    parts = [sums[y + k, h, pl.ds(32 * t + j, 8, stride=4), :] for j in range(4)]
                    dst[h, y + k + D, pl.ds(CX0 + 8 * t, 8), :] = 0.25 * (
                        (parts[0] + parts[1]) + (parts[2] + parts[3])
                    )

    rows_loop(*ys, body)


class Halo:
    def __init__(self, around, send, recv, halos):
        self.around, self.send, self.recv = around, send, recv
        self.base = sum(len(one.copies) for one in halos)
        self.copies = []
        halos.append(self)

    def add(self, buffer, size, y0, x0, dy, dx, ys, xs):
        n = self.base + len(self.copies)
        self.copies.append(
            pltpu.make_async_remote_copy(
                src_ref=buffer.at[:, pl.ds(y0 + ys[0], ys[1]), pl.ds(x0 + xs[0], xs[1]), :],
                dst_ref=buffer.at[
                    :, pl.ds(y0 + ys[0] - dy * size, ys[1]), pl.ds(x0 + xs[0] - dx * size, xs[1]), :
                ],
                send_sem=self.send.at[n],
                recv_sem=self.recv.at[n],
                device_id=self.around(dy, dx),
                device_id_type=pl.DeviceIdType.MESH,
            )
        )

    def edges(self, buffer, size, y0, x0, depths, along):
        low, high = depths
        along = (along[0], along[1] - along[0])
        for d in (1, -1):
            across = (size - high if d > 0 else low, high - low)
            self.add(buffer, size, y0, x0, 0, d, along, across)
            self.add(buffer, size, y0, x0, d, 0, across, along)

    def corners(self, buffer, size, y0, x0, rectangles):
        for (ya, yb), (xa, xb) in rectangles:
            for dy in (1, -1):
                for dx in (1, -1):
                    ys = (size - yb if dy > 0 else ya, yb - ya)
                    xs = (size - xb if dx > 0 else xa, xb - xa)
                    self.add(buffer, size, y0, x0, dy, dx, ys, xs)

    def relayed(self, buffer, size, y0, x0, rectangles):
        for (ya, yb), (xa, xb) in rectangles:
            for d in (1, -1):
                near_y = (size - yb if d > 0 else ya, yb - ya)
                near_x = (size - xb if d > 0 else xa, xb - xa)
                far_y = (size + ya if d > 0 else -yb, yb - ya)
                far_x = (-xb if d > 0 else size + xa, xb - xa)
                self.add(buffer, size, y0, x0, d, 0, near_y, far_x)
                self.add(buffer, size, y0, x0, 0, d, far_y, near_x)

    def start(self):
        for c in self.copies:
            c.start()

    def arrive(self):
        for c in self.copies:
            c.wait_recv()

    def sent(self):
        for c in self.copies:
            c.wait_send()


def first_kernel(
    right, guess, mass, v3, r, w, e, m, u, v1, v2, cl, cm, cw, ca, cb, sums, local, send, recv
):
    npy, npx = lax.axis_size("py"), lax.axis_size("px")
    py, px = lax.axis_index("py"), lax.axis_index("px")

    def around(dy, dx):
        return {"py": lax.rem(py + dy + npy, npy), "px": lax.rem(px + dx + npx, npx)}

    pieces = [((0, 4), (0, B)), ((B - 4, B), (0, B)), ((4, B - 4), (0, 8)), ((4, B - 4), (B - 8, B))]
    parts = [pieces, [((4, B - 4), (8, B - 8))]]
    whole = [[((0, B), (0, B))], []]
    loads = {}
    for part in range(2):
        for i, (src, dst) in enumerate(((guess, u), (right, r), (mass, m))):
            loads[i, part] = [
                pltpu.make_async_copy(
                    src.at[pl.ds(ya, yb - ya), pl.ds(xa, xb - xa), pl.ds(h * L, L)],
                    dst.at[h, pl.ds(Y0 + ya, yb - ya), pl.ds(X0 + xa, xb - xa), :],
                    local.at[i, 4 * part + n, h],
                )
                for n, ((ya, yb), (xa, xb)) in enumerate(whole[part])
                for h in range(H)
            ]
    for key in ((0, 0), (1, 0), (2, 0), (0, 1)):
        for c in loads[key]:
            c.start()

    def loaded(i, part):
        for c in loads[i, part]:
            c.wait()

    barrier = pltpu.get_barrier_semaphore()
    ring = [(dy, dx) for dy in (-1, 0, 1) for dx in (-1, 0, 1) if (dy, dx) != (0, 0)]
    for dy, dx in ring:
        pl.semaphore_signal(
            barrier, inc=1, device_id=around(dy, dx), device_id_type=pl.DeviceIdType.MESH
        )
    pl.semaphore_wait(barrier, len(ring))

    halos = []

    def halo(buffer, size, y0, x0, depths, rectangles):
        one = Halo(around, send, recv, halos)
        one.corners(buffer, size, y0, x0, rectangles)
        one.edges(buffer, size, y0, x0, depths, (0, size))
        return one

    square = lambda n: [((0, n), (0, n))]
    fine = lambda buffer, depths, rectangles: halo(buffer, B, Y0, X0, depths, rectangles)
    wedge = [((n, min(n + 2, D)), (0, D - n)) for n in range(0, D, 2)]

    loaded(0, 0)
    u_halo = fine(u, (0, 3), square(2))
    u_halo.start()
    loaded(1, 0)
    r_halo = fine(r, (0, 2), square(2))
    r_halo.start()
    loaded(2, 0)
    m_halo = fine(m, (0, 2), square(2))
    m_halo.start()

    def mass_rows(y, g):
        for k in range(g):
            for h in range(H):
                for x in tiles(0, B):
                    parts = [m[h, Y0 + 4 * (y + k) + j, pl.ds(X0 + x, 8), :] for j in range(4)]
                    sums[y + k, h, pl.ds(x, 8), :] = (parts[0] + parts[1]) + (parts[2] + parts[3])

    loaded(2, 1)
    rows_loop(0, C, mass_rows, 1)
    block_sums(cm, sums, (0, C))
    cm_halo = halo(cm, C, D, CX0, (0, D), [])
    cm_halo.start()
    m_more = fine(m, (2, 3), [])
    m_more.start()

    def defect(ys, xs):
        def body(y, g):
            for k in range(g):
                for h in range(H):
                    for x in tiles(*xs):
                        centre, near = near_sum(v2, h, Y0 + 4 * (y + k), X0 + x, 4)
                        parts = []
                        for j in range(4):
                            at = (h, Y0 + 4 * (y + k) + j, pl.ds(X0 + x, 8), slice(None))
                            parts.append(r[at] + near[j] - (4.0 + m[at]) * centre[j])
                        sums[y + k, h, pl.ds(x, 8), :] = (parts[0] + parts[1]) + (
                            parts[2] + parts[3]
                        )

        rows_loop(*ys, body, 1)

    weigh(w, m, (0, B), (0, B))
    loaded(0, 1)
    loaded(1, 1)
    sweep(v1, u, r, w, (2, B - 2), (2, B - 2))
    sweep(v2, v1, r, w, (3, B - 3), (3, B - 3))
    defect((1, C - 1), (4, B - 4))

    u_halo.arrive()
    r_halo.arrive()
    m_halo.arrive()
    for ys in ((-2, 0), (B, B + 2)):
        weigh(w, m, ys, (-2, B + 2))
    for xs in ((-2, 6), (B - 6, B + 2)):
        weigh(w, m, (0, B), xs)
    for ys in ((-2, 2), (B - 2, B + 2)):
        sweep(v1, u, r, w, ys, (-2, B + 2))
    for xs in ((-2, 6), (B - 6, B + 2)):
        sweep(v1, u, r, w, (2, B - 2), xs)
    for ys in ((-1, 3), (B - 3, B + 1)):
        sweep(v2, v1, r, w, ys, (0, B))
    for xs in ((-1, 7), (B - 7, B + 1)):
        sweep(v2, v1, r, w, (0, B), xs)
    for ys in ((0, 1), (C - 1, C)):
        defect(ys, (0, B))
    for xs in ((0, 8), (B - 8, B)):
        defect((1, C - 1), xs)
    block_sums(cl, sums, (0, C))
    cl_halo = halo(cl, C, D, CX0, (0, D), wedge)
    cl_halo.start()

    cm_halo.arrive()
    cm_far = Halo(around, send, recv, halos)
    cm_far.relayed(cm, C, D, CX0, wedge)
    cm_far.start()
    sweep(v3, v2, r, w, (0, B), (0, B))
    v3_halo = fine(v3, (0, 3), square(2))
    v3_halo.start()
    weigh(cw, cm, (0, C), (-D, C + D), D, CX0)
    for ys in ((-D, 0), (C, C + D)):
        weigh(cw, cm, ys, (0, C), D, CX0)
    cm_far.arrive()
    for ys in ((-D, 0), (C, C + D)):
        for xs in ((-D, 0), (C, C + D)):
            weigh(cw, cm, ys, xs, D, CX0)
    cl_halo.arrive()

    def first_coarse(y, g):
        for h in range(H):
            for x in tiles(-D, C + D):
                for k in range(g):
                    at = (h, y + D + k, pl.ds(x + CX0, 8), slice(None))
                    ca[at] = cw[at] * cl[at]

    rows_loop(-D, C + D, first_coarse, 2)
    here, there = ca, cb
    for n in range(D - 1, 0, -1):
        sweep(there, here, cl, cw, (-n, C + n), (-n, C + n), D, CX0)
        here, there = there, here

    def spread(y, g):
        for k in range(g):
            for h in range(H):
                for t in range(3):
                    value = here[h, y + k + D, pl.ds(CX0 - 1 + 8 * t, 8), :]
                    for j in range(4):
                        e[h, y + k + 2, pl.ds(EX0 - 4 + 32 * t + j, 8, stride=4), :] = value

    rows_loop(-1, C + 1, spread, 1)

    m_more.arrive()
    for ys in ((-3, -2), (B + 2, B + 3)):
        weigh(w, m, ys, (0, B))
    for xs in ((-3, 5), (B - 5, B + 3)):
        weigh(w, m, (0, B), xs)
    v3_halo.arrive()
    for one in halos:
        one.sent()


def second_kernel(v3, r, w, e, mass, corrected, remaining, a, b, m, sem, local):
    loads = [
        pltpu.make_async_copy(mass.at[:, :, pl.ds(h * L, L)], m.at[h], local.at[h])
        for h in range(H)
    ]
    for c in loads:
        c.start()

    def correct(y, g):
        for h in range(H):
            for x in tiles(-4, B + 4):
                at = lambda n, s=0: e[h, y + 2 + n, pl.ds(EX0 + x + s, 8), :]
                here, up, down = at(0), at(-1), at(1)
                sides = at(0, -1) + at(0, 1)
                small = 0.2 * here
                near = [sides + (up + here)] + [sides + (here + here)] * 2 + [sides + (here + down)]
                for k in range(4):
                    cell = (h, Y0 + 4 * y + k, pl.ds(X0 + x, 8), slice(None))
                    a[cell] = v3[cell] + (small + w[cell] * near[k])

    rows_loop(-1, C + 1, correct, 1)
    sweep(b, a, r, w, (-2, B + 2), (-2, B + 2))
    copies = []

    def put(src, dst, i, first, count):
        for h in range(H):
            c = pltpu.make_async_copy(
                src.at[h, pl.ds(Y0 + first, count), pl.ds(X0, B), :],
                dst.at[pl.ds(first, count), :, pl.ds(h * L, L)],
                sem.at[i, h],
            )
            c.start()
            copies.append(c)

    last = -1
    for i, upto in enumerate(FIRST_CUTS):
        sweep(a, b, r, w, (last, upto), (-1, B + 1))
        put(a, corrected, i, max(last, 0), min(upto, B) - max(last, 0))
        last = upto

    def rest(y, g):
        for h in range(H):
            for x in tiles(0, B):
                centre, near = near_sum(a, h, Y0 + y, X0 + x, g)
                for k in range(g):
                    at = (h, Y0 + y + k, pl.ds(X0 + x, 8), slice(None))
                    heavy = 4.0 + m[h, y + k, pl.ds(x, 8), :]
                    b[at] = r[at] + near[k] - heavy * centre[k]

    for c in loads:
        c.wait()
    last = 0
    for i, upto in enumerate(LAST_CUTS):
        rows_loop(last, upto, rest)
        put(b, remaining, len(FIRST_CUTS) + i, last, upto - last)
        last = upto
    for c in copies:
        c.wait()


def shards(right_side, first_guess, mass_term):
    f32 = jnp.float32
    copies = 4 * 8 + 2 * 24 + 4
    held = pl.pallas_call(
        first_kernel,
        out_shape=(*[pltpu.VMEM(FINE, f32)] * 3, pltpu.VMEM(SPREAD, f32)),
        in_specs=[ANY] * 3,
        out_specs=(VMEM,) * 4,
        scratch_shapes=[
            *[pltpu.VMEM(FINE, f32)] * 4,
            *[pltpu.VMEM(COARSE, f32)] * 5,
            pltpu.VMEM((C, H, B, L), f32),
            pltpu.SemaphoreType.DMA((3, 5, H)),
            pltpu.SemaphoreType.DMA((copies,)),
            pltpu.SemaphoreType.DMA((copies,)),
        ],
        compiler_params=pltpu.CompilerParams(
            collective_id=0, has_side_effects=True, vmem_limit_bytes=40 << 20
        ),
        name="first",
    )(right_side, first_guess, mass_term)
    held = [pltpu.with_memory_space_constraint(one, pltpu.VMEM) for one in held]
    mass_term = pltpu.with_memory_space_constraint(mass_term, pltpu.HBM)
    block = jax.ShapeDtypeStruct(right_side.shape, f32)
    return pl.pallas_call(
        second_kernel,
        out_shape=(block, block),
        in_specs=[VMEM] * 4 + [ANY],
        out_specs=(ANY, ANY),
        scratch_shapes=[
            *[pltpu.VMEM(FINE, f32)] * 2,
            pltpu.VMEM((H, B, B, L), f32),
            pltpu.SemaphoreType.DMA((len(FIRST_CUTS) + len(LAST_CUTS), H)),
            pltpu.SemaphoreType.DMA((H,)),
        ],
        compiler_params=pltpu.CompilerParams(vmem_limit_bytes=40 << 20),
        name="second",
    )(*held, mass_term)


def solution(mesh):
    spec = P(("shift", "py"), "px", None)
    return jax.shard_map(
        shards, mesh=mesh, in_specs=(spec,) * 3, out_specs=(spec,) * 2, check_vma=False
    )
```
